512 devices in a mesh: level: 2 (over z_lo), row: 16 (over y, core), col: 16 (over x, z_hi).
Axes of the slice: x: 4, y: 8, z: 8 (z_hi: 4, z_lo: 2; z = z_hi * 2 + z_lo), core: 2. Of those that a mesh axis runs over, the one named last changes fastest.
Arguments:
- initial: float32 [3, 2048, 16384], P(None, 'row', 'col'), may hold values from -0.75 to 0.75
Outputs:
- levels_out: float32 [2, 3, 2048, 16384], P('level', None, 'row', 'col')
The draws below stay inside these ranges and needn't reach their ends.
All inputs are finite; a program needn't handle non-finite values.
Results may differ from the reference program's by a relative error of at most 0.00002.
Values sent between devices are 32-bit elements; how exact they have to be, the bound alone decides.
A program may use at most 64 MiB of HBM per device.

```python
import jax
import jax.numpy as jnp
from jax import lax

STEPS = 8
NX = 2048
NY = 16384


def shard_levels(own_key, shape, split, smallest, top_value):
    def one(position, shards_of):
        draws = jax.random.uniform(jax.random.fold_in(jax.random.fold_in(own_key, 6), position), (shards_of,), jnp.float32, smallest / len(split), top_value / len(split))
        return jnp.repeat(jnp.exp(draws), shape[position] // shards_of).reshape((-1,) + (1,) * (len(shape) - position - 1))

    factor_of = one(*split[0])
    for cut in split[1:]:
        factor_of = factor_of * one(*cut)
    return factor_of


def centred(rng, shape, deviation, bound, pieces=(), held_as=jnp.bfloat16):
    entries = deviation * jax.random.normal(rng, shape, jnp.float32)
    if pieces:
        entries = entries * shard_levels(rng, shape, pieces, -0.22, 0.18)
    return jnp.clip(entries, -bound, bound).astype(held_as)


def setup_inputs(seed: int = 0) -> dict:
    key_list = jax.random.split(jax.random.key(seed), 2)
    return {
        "initial": centred(key_list[0], (3, NX, NY), 0.25, 0.75, ((1, 16), (2, 16)), jnp.float32),
    }


time_step = 0.1
gravity = 1.0
rotation = 0.2


def along_rows(values):
    return 0.5 * (jnp.roll(values, -1, axis=0) - jnp.roll(values, 1, axis=0))


def along_cols(values):
    return 0.5 * (jnp.roll(values, -1, axis=1) - jnp.roll(values, 1, axis=1))


def tendency(current):
    surface = current[0]
    eastward = current[1]
    northward = current[2]
    height = 1.0 + surface
    surface_rate = -(along_rows(height * eastward) + along_cols(height * northward))
    east_rate = -(eastward * along_rows(eastward) + northward * along_cols(eastward)) - gravity * along_rows(surface) + rotation * northward
    north_rate = -(eastward * along_rows(northward) + northward * along_cols(northward)) - gravity * along_cols(surface) - rotation * eastward
    return jnp.stack([surface_rate, east_rate, north_rate])


def reference(initial):
    def advance(moment, carry):
        predicted, corrected, predicted_rate = carry
        next_pred = predicted + time_step * predicted_rate
        next_rate = tendency(next_pred)
        corrected = corrected + time_step * tendency(corrected) + 0.5 * time_step * (next_rate - predicted_rate)
        return (next_pred, corrected, next_rate)

    start = initial.astype(jnp.float32)
    result = lax.fori_loop(0, STEPS, advance, (start, start, tendency(start)))
    return jnp.stack([result[0], result[1]])
```

```python
import functools

import jax
import jax.numpy as jnp
from jax import lax
from jax.experimental import pallas as pl
from jax.experimental.pallas import tpu as pltpu
from jax.sharding import PartitionSpec as P

STEPS = 8
TIME_STEP = 0.1
GRAVITY = 1.0
ROTATION = 0.2

HALF = 0.5 * TIME_STEP
SCALES = (HALF * HALF * GRAVITY, HALF, HALF)
REST = HALF * HALF * GRAVITY
TURN = TIME_STEP * ROTATION

ROWS = 128
COLS = 1024
TILES = COLS // 128
STRIP = 9
STRIPS = 16
PITCH = 11
FRONT = 16
SPAN = 128 + 2 * FRONT
WORDS = SPAN * PITCH
VMEM = pltpu.VMEM


def exchange_kernel(rows_n, cols_n, x, north, south, sides, corners,
                    top, bottom, left, right, packed, corner_out, local, send, recv):
    me_r, me_c = lax.axis_index("row"), lax.axis_index("col")
    up, down = lax.rem(me_r + rows_n - 1, rows_n), lax.rem(me_r + 1, rows_n)
    west, east = lax.rem(me_c + cols_n - 1, cols_n), lax.rem(me_c + 1, cols_n)
    places = [(up, me_c), (down, me_c), (me_r, west), (me_r, east), (up, west), (up, east), (down, west), (down, east)]
    ids = [{"row": r, "col": c} for r, c in places]
    barrier = pltpu.get_barrier_semaphore()
    for where in ids:
        pl.semaphore_signal(barrier, inc=1, device_id=where, device_id_type=pl.DeviceIdType.MESH)
    loads = [
        pltpu.make_async_copy(x.at[:, :, 0:128], left, local.at[0]),
        pltpu.make_async_copy(x.at[:, :, COLS - 128:COLS], right, local.at[1]),
        pltpu.make_async_copy(x.at[:, 0:16, :], top, local.at[2]),
        pltpu.make_async_copy(x.at[:, ROWS - 16:ROWS, :], bottom, local.at[3]),
    ]
    for load in loads:
        load.start()
    loads[0].wait()
    loads[1].wait()
    lane = lax.broadcasted_iota(jnp.int32, (16, 128), 1)
    for f in range(3):
        packed[0, f] = jnp.transpose(left[f])[0:16]
        packed[1, f] = jnp.transpose(right[f])[112:128]
    for k, (ref, row0, lane0) in enumerate(((left, 0, 0), (right, 0, 112), (left, ROWS - 16, 0), (right, ROWS - 16, 112))):
        out = ref[0, row0:row0 + 16]
        if lane0:
            out = pltpu.roll(out, 128 - lane0, 1)
        for f in (1, 2):
            piece = pltpu.roll(ref[f, row0:row0 + 16], (128 - lane0 + 16 * f) % 128, 1)
            out = jnp.where(lane < 16 * f, out, piece)
        corner_out[k] = out
    loads[2].wait()
    loads[3].wait()
    pl.semaphore_wait(barrier, 8)
    sends = []
    pieces = [
        (top, south), (bottom, north),
        (packed.at[0], sides.at[0]), (packed.at[1], sides.at[1]),
        (corner_out.at[0], corners.at[3]), (corner_out.at[1], corners.at[2]),
        (corner_out.at[2], corners.at[1]), (corner_out.at[3], corners.at[0]),
    ]
    for k, (src, dst) in enumerate(pieces):
        sends.append(pltpu.make_async_remote_copy(
            src_ref=src, dst_ref=dst, send_sem=send.at[k], recv_sem=recv.at[k],
            device_id=ids[k], device_id_type=pl.DeviceIdType.MESH))
    for k in (4, 5, 6, 7, 2, 3, 0, 1):
        sends[k].start()
    for one in sends:
        one.wait()


def exchange(x, rows_n, cols_n):
    f32 = jnp.float32
    any_spec = pl.BlockSpec(memory_space=pl.ANY)
    return pl.pallas_call(
        functools.partial(exchange_kernel, rows_n, cols_n),
        out_shape=(
            jax.ShapeDtypeStruct((3, 16, COLS), f32),
            jax.ShapeDtypeStruct((3, 16, COLS), f32),
            jax.ShapeDtypeStruct((2, 3, 16, 128), f32),
            jax.ShapeDtypeStruct((4, 16, 128), f32),
        ),
        in_specs=[any_spec],
        out_specs=(any_spec,) * 4,
        scratch_shapes=[
            VMEM((3, 16, COLS), f32),
            VMEM((3, 16, COLS), f32),
            VMEM((3, ROWS, 128), f32),
            VMEM((3, ROWS, 128), f32),
            VMEM((2, 3, 16, 128), f32),
            VMEM((4, 16, 128), f32),
            pltpu.SemaphoreType.DMA((4,)),
            pltpu.SemaphoreType.DMA((8,)),
            pltpu.SemaphoreType.DMA((8,)),
        ],
        compiler_params=pltpu.CompilerParams(collective_id=0, has_side_effects=True),
    )(x)


def word(q, r):
    return (q + FRONT) * PITCH + r + 1


def take(ref, q, r):
    return ref[pl.ds(word(q, r), 8, stride=PITCH), :]


def put(ref, q, r, value):
    ref[pl.ds(word(q, r), 8, stride=PITCH), :] = value


def slopes(state, q0, act):
    e_ref, u_ref, v_ref, w_ref = state

    def load(r):
        e, u, v = take(e_ref, q0, r), take(u_ref, q0, r), take(v_ref, q0, r)
        return e, u, v, (e + REST) * u

    below, here = load(-1), load(0)
    for r in range(STRIP):
        above = load(r + 1)
        e, u, v, _ = here
        de, du, dv, dw = (a - b for a, b in zip(above, below))
        ye = take(e_ref, q0 + 1, r) - take(e_ref, q0 - 1, r)
        yu = take(u_ref, q0 + 1, r) - take(u_ref, q0 - 1, r)
        yv = take(v_ref, q0 + 1, r) - take(v_ref, q0 - 1, r)
        yw = take(w_ref, q0 + 1, r) - take(w_ref, q0 - 1, r)
        ge = dw + yw
        gu = (u * du + v * (yu - TURN)) + de
        gv = (u * (dv + TURN) + v * yv) + ye
        act(r, (e, u, v), (ge, gu, gv))
        below, here = here, above


def edges(refs, q0):
    for ref in refs:
        put(ref, q0, -1, pltpu.roll(take(ref, q0, STRIP - 1), TILES, 1))
        put(ref, q0, STRIP, pltpu.roll(take(ref, q0, 0), 128 - TILES, 1))


def sweep(first, blocks, work, late, unroll):
    trips, rest = divmod(blocks, unroll)

    def trip(start, count, before):
        for k in range(count):
            work(start + 8 * k)
        for k in range(before):
            late(start + 8 * (k - before))

    trip(first, unroll, 0)

    def step(i, carry):
        trip(first + 8 * unroll * i, unroll, unroll)
        return carry

    lax.fori_loop(1, trips, step, 0)
    last = first + 8 * unroll * trips
    if rest:
        trip(last, rest, unroll)
        left = [last + 8 * k for k in range(rest)]
    else:
        left = [last + 8 * (k - unroll) for k in range(unroll)]

    def finish():
        for q in left:
            late(q)

    return finish


def window_kernel(x, north, south, sides, corners, out,
                  grid, turned, side_in, corner_in, pe, pu, pv, pw, qe, qu, qv, qw,
                  ce, cu, cv, cw, de, du, dv, sems, out_sems):
    level = lax.axis_index("level")
    copies = []

    def fetch(src, dst):
        copies.append(pltpu.make_async_copy(src, dst, sems.at[len(copies)]))
        copies[-1].start()

    view = x.reshape(3, 16, 8, COLS)
    n_view, s_view = north.reshape(3, 2, 8, COLS), south.reshape(3, 2, 8, COLS)
    for c in range(TILES):
        cut = slice(128 * c, 128 * c + 128)
        fetch(view.at[:, :, :, cut], grid.at[:, 2:18, c + 1])
        fetch(n_view.at[:, :, :, cut], grid.at[:, 0:2, c + 1])
        fetch(s_view.at[:, :, :, cut], grid.at[:, 18:20, c + 1])
    fetch(sides.at[0], side_in.at[:, 0:16])
    fetch(sides.at[1], side_in.at[:, 112:128])
    fetch(corners, corner_in)
    for copy in copies:
        copy.wait()

    lane8 = lax.broadcasted_iota(jnp.int32, (8, 128), 1)
    for f in range(3):
        beside = jnp.transpose(side_in[f])
        for t in range(16):
            part = beside[8 * t:8 * t + 8]
            grid[f, t + 2, 0] = part
            grid[f, t + 2, TILES + 1] = part
        for t in range(2):
            for k, place in ((0, 0), (2, 18)):
                west = corner_in[k, 8 * t:8 * t + 8]
                east = corner_in[k + 1, 8 * t:8 * t + 8]
                west = pltpu.roll(west, (112 - 16 * f) % 128, 1)
                if f:
                    east = pltpu.roll(east, 128 - 16 * f, 1)
                grid[f, place + t, 0] = west
                grid[f, place + t, TILES + 1] = east

    flat = grid.reshape(3, 20 * 10 * 8, 128)

    def tile_row(f, i, shift):
        i = i + 16
        return flat[f, pl.ds((i // 8) * 80 + 8 * (1 + shift) + i % 8, TILES, stride=8), :]

    for r in range(-1, STRIP + 1):
        for f, ref in enumerate((pe, pu, pv)):
            here, beside = [], []
            for s in range(STRIPS):
                i = s * STRIP + r - 8
                here.append(tile_row(f, i, 0))
                beside.append(jnp.where(lane8 >= 64, tile_row(f, i, -1), tile_row(f, i, 1)))
            here = jnp.transpose(jnp.concatenate(here, axis=0)) * SCALES[f]
            beside = jnp.transpose(jnp.concatenate(beside, axis=0)) * SCALES[f]
            for k in range(16):
                put(ref, 8 * k, r, here[8 * k:8 * k + 8])
            put(ref, -16, r, beside[112:120])
            put(ref, -8, r, beside[120:128])
            put(ref, 128, r, beside[0:8])
            put(ref, 136, r, beside[8:16])

    def weigh(i, carry):
        at = pl.ds(pl.multiple_of(i * 8 * 11, 8), 8 * 11)
        pw[at, :] = (pe[at, :] + REST) * pv[at, :]
        return carry

    lax.fori_loop(0, SPAN // 8, weigh, 0)

    def keep(refs, q, r, values):
        for ref, value in zip(refs, values):
            put(ref, q, r, value)

    def weighed(values):
        e, u, v = values
        return e, u, v, (e + REST) * v

    a_state, b_state = (pe, pu, pv, pw), (qe, qu, qv, qw)
    c_state, d_state = (ce, cu, cv, cw), (de, du, dv)
    nothing = lambda q: None

    def predict(now, then, m, with_c):
        def work(q0):
            def act(r, own, change):
                new = tuple(p - g for p, g in zip(own, change))
                keep(then, q0, r, weighed(new))
                if with_c and m == 0:
                    keep(d_state, q0, r, tuple(p - 0.5 * g for p, g in zip(own, change)))
                elif with_c:
                    mid = tuple(take(ref, q0, r) - 0.5 * g for ref, g in zip(d_state, change))
                    keep(c_state, q0, r, weighed(mid))

            slopes(now, q0, act)

        def late(q0):
            if with_c and m:
                edges(c_state[:3], q0)
            edges(then[:3], q0)

        reach = STEPS - m
        return sweep(-reach, (128 + 2 * reach + 7) // 8, work, late, 2)

    def correct(m):
        def work(q0):
            def act(r, own, change):
                keep(d_state, q0, r, tuple(take(ref, q0, r) - g for ref, g in zip(d_state, change)))

            slopes(c_state, q0, act)

        reach = STEPS - 1 - m
        return sweep(-reach, (128 + 2 * reach + 7) // 8, work, nothing, 2)

    def last():
        def work(q0):
            def act(r, own, change):
                keep(c_state, q0, r, tuple(take(ref, q0, r) - 0.5 * g for ref, g in zip(d_state, change)))

            slopes(a_state, q0, act)

        sweep(0, 16, work, nothing, 2)

    def emit(refs):
        done = []
        for f, ref in enumerate(refs):
            for r in range(STRIP):
                block = jnp.concatenate([take(ref, 8 * k, r) for k in range(16)], axis=0)
                block = jnp.transpose(block) * (1.0 / SCALES[f])
                for s in range(STRIPS):
                    i = s * STRIP + r - 8
                    if 0 <= i < ROWS:
                        flat[f, pl.ds((i // 8) * 80 + 8 + i % 8, TILES, stride=8), :] = block[8 * s:8 * s + 8]
            target = out.reshape(1, 3, 16, 8, COLS)
            for c in range(TILES):
                copy = pltpu.make_async_copy(
                    grid.at[f, 0:16, c + 1], target.at[0, f, :, :, 128 * c:128 * c + 128], out_sems.at[f * TILES + c])
                copy.start()
                done.append(copy)
        for copy in done:
            copy.wait()

    @pl.when(level == 0)
    def _():
        for m in range(STEPS):
            now, then = (a_state, b_state) if m % 2 == 0 else (b_state, a_state)
            predict(now, then, m, False)()
        emit(a_state[:3])

    @pl.when(level == 1)
    def _():
        for m in range(STEPS):
            now, then = (a_state, b_state) if m % 2 == 0 else (b_state, a_state)
            predict(now, then, m, True)()
            if m:
                correct(m)
        last()
        emit(c_state[:3])


def window(x, north, south, sides, corners):
    f32 = jnp.float32
    any_spec = pl.BlockSpec(memory_space=pl.ANY)
    return pl.pallas_call(
        window_kernel,
        out_shape=jax.ShapeDtypeStruct((1, 3, ROWS, COLS), f32),
        in_specs=[any_spec] * 5,
        out_specs=any_spec,
        scratch_shapes=[
            VMEM((3, 20, 10, 8, 128), f32),
            VMEM((8, 128), f32),
            VMEM((3, 128, 128), f32),
            VMEM((4, 16, 128), f32),
        ] + [VMEM((WORDS, 128), f32) for _ in range(15)] + [
            pltpu.SemaphoreType.DMA((3 * TILES + 3,)),
            pltpu.SemaphoreType.DMA((3 * TILES,)),
        ],
        compiler_params=pltpu.CompilerParams(vmem_limit_bytes=48 * 1024 * 1024),
    )(x, north, south, sides, corners)


def solution(mesh):
    rows_n, cols_n = mesh.shape["row"], mesh.shape["col"]

    def body(x):
        return window(x, *exchange(x, rows_n, cols_n))

    return jax.shard_map(
        body,
        mesh=mesh,
        in_specs=(P(None, "row", "col"),),
        out_specs=P("level", None, "row", "col"),
        check_vma=False,
    )
```

```python
import functools

import jax
import jax.numpy as jnp
from jax import lax
from jax.experimental import pallas as pl
from jax.experimental.pallas import tpu as pltpu
from jax.sharding import PartitionSpec as P

STEPS = 8
TIME_STEP = 0.1
GRAVITY = 1.0
ROTATION = 0.2

HALF = 0.5 * TIME_STEP
SCALES = (HALF * HALF * GRAVITY, HALF, HALF)
REST = HALF * HALF * GRAVITY
TURN = TIME_STEP * ROTATION

ROWS = 128
COLS = 1024
TILES = COLS // 128
STRIP = 9
STRIPS = 16
PITCH = 9
RIM = 3
FRONT = 16
SPAN = 128 + 2 * FRONT
WORDS = SPAN * PITCH
VMEM = pltpu.VMEM


def exchange_kernel(rows_n, cols_n, x, north, south, sides, corners,
                    top, bottom, left, right, packed, corner_out, local, send, recv):
    me_r, me_c = lax.axis_index("row"), lax.axis_index("col")
    up, down = lax.rem(me_r + rows_n - 1, rows_n), lax.rem(me_r + 1, rows_n)
    west, east = lax.rem(me_c + cols_n - 1, cols_n), lax.rem(me_c + 1, cols_n)
    places = [(up, me_c), (down, me_c), (me_r, west), (me_r, east), (up, west), (up, east), (down, west), (down, east)]
    ids = [{"row": r, "col": c} for r, c in places]
    barrier = pltpu.get_barrier_semaphore()
    for where in ids:
        pl.semaphore_signal(barrier, inc=1, device_id=where, device_id_type=pl.DeviceIdType.MESH)
    loads = [
        pltpu.make_async_copy(x.at[:, :, 0:128], left, local.at[0]),
        pltpu.make_async_copy(x.at[:, :, COLS - 128:COLS], right, local.at[1]),
        pltpu.make_async_copy(x.at[:, 0:16, :], top, local.at[2]),
        pltpu.make_async_copy(x.at[:, ROWS - 16:ROWS, :], bottom, local.at[3]),
    ]
    for load in loads:
        load.start()
    loads[0].wait()
    loads[1].wait()
    lane = lax.broadcasted_iota(jnp.int32, (16, 128), 1)
    for f in range(3):
        packed[0, f] = jnp.transpose(left[f])[0:16]
        packed[1, f] = jnp.transpose(right[f])[112:128]
    for k, (ref, row0, lane0) in enumerate(((left, 0, 0), (right, 0, 112), (left, ROWS - 16, 0), (right, ROWS - 16, 112))):
        out = ref[0, row0:row0 + 16]
        if lane0:
            out = pltpu.roll(out, 128 - lane0, 1)
        for f in (1, 2):
            piece = pltpu.roll(ref[f, row0:row0 + 16], (128 - lane0 + 16 * f) % 128, 1)
            out = jnp.where(lane < 16 * f, out, piece)
        corner_out[k] = out
    loads[2].wait()
    loads[3].wait()
    pl.semaphore_wait(barrier, 8)
    sends = []
    pieces = [
        (top, south), (bottom, north),
        (packed.at[0], sides.at[0]), (packed.at[1], sides.at[1]),
        (corner_out.at[0], corners.at[3]), (corner_out.at[1], corners.at[2]),
        (corner_out.at[2], corners.at[1]), (corner_out.at[3], corners.at[0]),
    ]
    for k, (src, dst) in enumerate(pieces):
        sends.append(pltpu.make_async_remote_copy(
            src_ref=src, dst_ref=dst, send_sem=send.at[k], recv_sem=recv.at[k],
            device_id=ids[k], device_id_type=pl.DeviceIdType.MESH))
    for k in (4, 5, 6, 7, 2, 3, 0, 1):
        sends[k].start()
    for one in sends:
        one.wait()


def exchange(x, rows_n, cols_n):
    f32 = jnp.float32
    any_spec = pl.BlockSpec(memory_space=pltpu.HBM)
    return pl.pallas_call(
        functools.partial(exchange_kernel, rows_n, cols_n),
        out_shape=(
            jax.ShapeDtypeStruct((3, 16, COLS), f32),
            jax.ShapeDtypeStruct((3, 16, COLS), f32),
            jax.ShapeDtypeStruct((2, 3, 16, 128), f32),
            jax.ShapeDtypeStruct((4, 16, 128), f32),
        ),
        in_specs=[any_spec],
        out_specs=(any_spec,) * 4,
        scratch_shapes=[
            VMEM((3, 16, COLS), f32),
            VMEM((3, 16, COLS), f32),
            VMEM((3, ROWS, 128), f32),
            VMEM((3, ROWS, 128), f32),
            VMEM((2, 3, 16, 128), f32),
            VMEM((4, 16, 128), f32),
            pltpu.SemaphoreType.DMA((4,)),
            pltpu.SemaphoreType.DMA((8,)),
            pltpu.SemaphoreType.DMA((8,)),
        ],
        compiler_params=pltpu.CompilerParams(collective_id=0, has_side_effects=True),
    )(x)


def cut_of(q, r):
    if 0 <= r < STRIP:
        return 0, pl.ds((q + FRONT) * PITCH + r, 8, stride=PITCH)
    return 1, pl.ds((q + FRONT) * RIM + (r > 0), 8, stride=RIM)


def take(ref, q, r):
    which, cut = cut_of(q, r)
    return ref[which][cut, :]


def put(ref, q, r, value):
    which, cut = cut_of(q, r)
    ref[which][cut, :] = value


def slopes(state, q0, act):
    e_ref, u_ref, v_ref, w_ref = state

    def load(r):
        e, u, v = take(e_ref, q0, r), take(u_ref, q0, r), take(v_ref, q0, r)
        return e, u, v, (e + REST) * u

    below, here = load(-1), load(0)
    for r in range(STRIP):
        above = load(r + 1)
        e, u, v, _ = here
        de, du, dv, dw = (a - b for a, b in zip(above, below))
        ye = take(e_ref, q0 + 1, r) - take(e_ref, q0 - 1, r)
        yu = take(u_ref, q0 + 1, r) - take(u_ref, q0 - 1, r)
        yv = take(v_ref, q0 + 1, r) - take(v_ref, q0 - 1, r)
        yw = take(w_ref, q0 + 1, r) - take(w_ref, q0 - 1, r)
        ge = dw + yw
        gu = (u * du + v * (yu - TURN)) + de
        gv = (u * (dv + TURN) + v * yv) + ye
        act(r, (e, u, v), (ge, gu, gv))
        below, here = here, above


def edges(refs, q0):
    rows = [(ref, pltpu.roll(take(ref, q0, STRIP - 1), TILES, 1), pltpu.roll(take(ref, q0, 0), 128 - TILES, 1)) for ref in refs]

    def store():
        for ref, low, high in rows:
            put(ref, q0, -1, low)
            put(ref, q0, STRIP, high)

    return store


def sweep(first, blocks, work, late, unroll):
    trips, rest = divmod(blocks, unroll)

    def trip(start, count, before):
        stores = [late(start + 8 * (k - before)) for k in range(before)]
        for k in range(count):
            work(start + 8 * k)
        for store in stores:
            store()

    trip(first, unroll, 0)

    def step(i, carry):
        trip(first + 8 * unroll * i, unroll, unroll)
        return carry

    lax.fori_loop(1, trips, step, 0)
    last = first + 8 * unroll * trips
    if rest:
        trip(last, rest, unroll)
        left = [last + 8 * k for k in range(rest)]
    else:
        left = [last + 8 * (k - unroll) for k in range(unroll)]

    def finish():
        for store in [late(q) for q in left]:
            store()

    return finish


def window_kernel(x, north, south, sides, corners, out,
                  grid, side_in, corner_in, sems, out_sems, *state):
    level = lax.axis_index("level")
    copies = []
    fields, rims = list(state[:18]), list(state[18:])
    pe, pu, pv, qe, qu, qv, ce, cu, cv = zip(fields[:9], rims)
    pw, qw, cw, de, du, dv, fe, fu, fv = ((one,) for one in fields[9:])

    def fetch(src, dst):
        copies.append(pltpu.make_async_copy(src, dst, sems.at[len(copies)]))
        copies[-1].start()

    view = x.reshape(3, 16, 8, COLS)
    n_view, s_view = north.reshape(3, 2, 8, COLS), south.reshape(3, 2, 8, COLS)
    for c in range(TILES):
        cut = slice(128 * c, 128 * c + 128)
        fetch(view.at[:, :, :, cut], grid.at[:, 2:18, c + 1])
        fetch(n_view.at[:, :, :, cut], grid.at[:, 0:2, c + 1])
        fetch(s_view.at[:, :, :, cut], grid.at[:, 18:20, c + 1])
    fetch(sides.at[0], side_in.at[:, 0:16])
    fetch(sides.at[1], side_in.at[:, 112:128])
    fetch(corners, corner_in)
    for copy in copies:
        copy.wait()

    lane8 = lax.broadcasted_iota(jnp.int32, (8, 128), 1)
    for f in range(3):
        beside = jnp.transpose(side_in[f])
        for t in range(16):
            part = beside[8 * t:8 * t + 8]
            grid[f, t + 2, 0] = part
            grid[f, t + 2, TILES + 1] = part
        for t in range(2):
            for k, place in ((0, 0), (2, 18)):
                west = corner_in[k, 8 * t:8 * t + 8]
                east = corner_in[k + 1, 8 * t:8 * t + 8]
                west = pltpu.roll(west, (112 - 16 * f) % 128, 1)
                if f:
                    east = pltpu.roll(east, 128 - 16 * f, 1)
                grid[f, place + t, 0] = west
                grid[f, place + t, TILES + 1] = east

    flat = grid.reshape(3, 20 * 10 * 8, 128)

    def tile_row(f, i, shift):
        i = i + 16
        return flat[f, pl.ds((i // 8) * 80 + 8 * (1 + shift) + i % 8, TILES, stride=8), :]

    for r in range(-1, STRIP + 1):
        for f, ref in enumerate((pe, pu, pv)):
            here, beside = [], []
            for s in range(STRIPS):
                i = s * STRIP + r - 8
                here.append(tile_row(f, i, 0))
                beside.append(jnp.where(lane8 >= 64, tile_row(f, i, -1), tile_row(f, i, 1)))
            here = jnp.transpose(jnp.concatenate(here, axis=0)) * SCALES[f]
            beside = jnp.transpose(jnp.concatenate(beside, axis=0)) * SCALES[f]
            for k in range(16):
                put(ref, 8 * k, r, here[8 * k:8 * k + 8])
            put(ref, -16, r, beside[112:120])
            put(ref, -8, r, beside[120:128])
            put(ref, 128, r, beside[0:8])
            put(ref, 136, r, beside[8:16])

    def weigh(i, carry):
        at = pl.ds(pl.multiple_of(i * 8 * PITCH, 8), 8 * PITCH)
        pw[0][at, :] = (pe[0][at, :] + REST) * pv[0][at, :]
        return carry

    lax.fori_loop(0, SPAN // 8, weigh, 0)

    def keep(refs, q, r, values):
        for ref, value in zip(refs, values):
            put(ref, q, r, value)

    def weighed(values):
        e, u, v = values
        return e, u, v, (e + REST) * v

    a_state, b_state = (pe, pu, pv, pw), (qe, qu, qv, qw)
    c_state, d_states = (ce, cu, cv, cw), ((de, du, dv), (fe, fu, fv))
    nothing = lambda q: lambda: None

    def predict(now, then, m, with_c):
        def work(q0):
            def act(r, own, change):
                new = tuple(p - g for p, g in zip(own, change))
                keep(then, q0, r, weighed(new))
                if with_c and m == 0:
                    keep(d_states[1], q0, r, tuple(p - 0.5 * g for p, g in zip(own, change)))
                elif with_c:
                    mid = tuple(take(ref, q0, r) - 0.5 * g for ref, g in zip(d_states[m % 2], change))
                    keep(c_state, q0, r, weighed(mid))

            slopes(now, q0, act)

        def late(q0):
            return edges(c_state[:3] + then[:3] if with_c and m else then[:3], q0)

        reach = STEPS - m
        return sweep(-reach, (128 + 2 * reach + 7) // 8, work, late, 2 if with_c else 2)

    def correct(m):
        def work(q0):
            def act(r, own, change):
                keep(d_states[(m + 1) % 2], q0, r, tuple(take(ref, q0, r) - g for ref, g in zip(d_states[m % 2], change)))

            slopes(c_state, q0, act)

        reach = STEPS - 1 - m
        return sweep(-reach, (128 + 2 * reach + 7) // 8, work, nothing, 2)

    def last():
        def work(q0):
            def act(r, own, change):
                keep(c_state, q0, r, tuple(take(ref, q0, r) - 0.5 * g for ref, g in zip(d_states[0], change)))

            slopes(a_state, q0, act)

        sweep(0, 16, work, nothing, 2)

    def emit(refs):
        done = []
        for f, ref in enumerate(refs):
            for r in range(STRIP):
                block = jnp.concatenate([take(ref, 8 * k, r) for k in range(16)], axis=0)
                block = jnp.transpose(block) * (1.0 / SCALES[f])
                for s in range(STRIPS):
                    i = s * STRIP + r - 8
                    if 0 <= i < ROWS:
                        flat[f, pl.ds((i // 8) * 80 + 8 + i % 8, TILES, stride=8), :] = block[8 * s:8 * s + 8]
            target = out.reshape(1, 3, 16, 8, COLS)
            for c in range(TILES):
                copy = pltpu.make_async_copy(
                    grid.at[f, 0:16, c + 1], target.at[0, f, :, :, 128 * c:128 * c + 128], out_sems.at[f * TILES + c])
                copy.start()
                done.append(copy)
        for copy in done:
            copy.wait()

    @pl.when(level == 0)
    def _():
        for m in range(STEPS):
            now, then = (a_state, b_state) if m % 2 == 0 else (b_state, a_state)
            predict(now, then, m, False)()
        emit(a_state[:3])

    @pl.when(level == 1)
    def _():
        for m in range(STEPS):
            now, then = (a_state, b_state) if m % 2 == 0 else (b_state, a_state)
            predict(now, then, m, True)()
            if m:
                correct(m)
        last()
        emit(c_state[:3])


def window(x, north, south, sides, corners):
    f32 = jnp.float32
    any_spec = pl.BlockSpec(memory_space=pltpu.HBM)
    return pl.pallas_call(
        window_kernel,
        out_shape=jax.ShapeDtypeStruct((1, 3, ROWS, COLS), f32),
        in_specs=[any_spec] * 5,
        out_specs=any_spec,
        scratch_shapes=[
            VMEM((3, 20, 10, 8, 128), f32),
            VMEM((3, 128, 128), f32),
            VMEM((4, 16, 128), f32),
            pltpu.SemaphoreType.DMA((3 * TILES + 3,)),
            pltpu.SemaphoreType.DMA((3 * TILES,)),
        ] + [VMEM((WORDS, 128), f32) for _ in range(18)] + [VMEM((SPAN * RIM, 128), f32) for _ in range(9)],
        compiler_params=pltpu.CompilerParams(),
    )(x, north, south, sides, corners)


def solution(mesh):
    rows_n, cols_n = mesh.shape["row"], mesh.shape["col"]

    def body(x):
        return window(x, *exchange(x, rows_n, cols_n))

    return jax.shard_map(
        body,
        mesh=mesh,
        in_specs=(P(None, "row", "col"),),
        out_specs=P("level", None, "row", "col"),
        check_vma=False,
    )
```

```python
import functools

import jax
import jax.numpy as jnp
from jax import lax
from jax.experimental import pallas as pl
from jax.experimental.pallas import tpu as pltpu
from jax.sharding import PartitionSpec as P

STEPS = 8
TIME_STEP = 0.1
GRAVITY = 1.0
ROTATION = 0.2

HALF = 0.5 * TIME_STEP
SCALES = (HALF * HALF * GRAVITY, HALF, HALF)
REST = HALF * HALF * GRAVITY
TURN = TIME_STEP * ROTATION

ROWS = 128
COLS = 1024
TILES = COLS // 128
STRIP = 9
STRIPS = 16
PITCH = 9
RIM = 3
FRONT = 16
SPAN = 128 + 2 * FRONT
WORDS = SPAN * PITCH
VMEM = pltpu.VMEM


def exchange_kernel(rows_n, cols_n, x, north, south, sides, corners,
                    top, bottom, left, right, side_out, corner_out, send, recv):
    me_r, me_c = lax.axis_index("row"), lax.axis_index("col")
    up, down = lax.rem(me_r + rows_n - 1, rows_n), lax.rem(me_r + 1, rows_n)
    west, east = lax.rem(me_c + cols_n - 1, cols_n), lax.rem(me_c + 1, cols_n)
    places = [(up, me_c), (down, me_c), (me_r, west), (me_r, east), (up, west), (up, east), (down, west), (down, east)]
    ids = [{"row": r, "col": c} for r, c in places]
    barrier = pltpu.get_barrier_semaphore()
    for where in ids:
        pl.semaphore_signal(barrier, inc=1, device_id=where, device_id_type=pl.DeviceIdType.MESH)
    lane = lax.broadcasted_iota(jnp.int32, (16, 128), 1)
    view = x.reshape(3, ROWS // 8, 8 * TILES, 128)
    for f in range(3):
        for k, ref in enumerate((left, right)):
            column = (TILES - 1) * k * 8
            ref[f] = view[f, :, column:column + 8, :].reshape(ROWS, 128)
    ends = (left, right)
    for f in range(3):
        side_out[0, 9 * f:9 * f + 9] = jnp.transpose(left[f])[0:9]
        side_out[1, 9 * f:9 * f + 9] = jnp.transpose(right[f])[119:128]
        top[f, 0:64] = x[f, 0:64]
        bottom[f, 0:64] = x[f, 8 * ROWS - 64:8 * ROWS]
        top[f, 64:72] = x[f, pl.ds(64, TILES, stride=8), :]
        bottom[f, 64:72] = x[f, pl.ds(8 * ROWS - 128 + 7, TILES, stride=8), :]
    for k, (ref, row0, lane0) in enumerate(((0, 0, 0), (1, 0, 112), (0, ROWS - 16, 0), (1, ROWS - 16, 112))):
        out = ends[ref][0, row0:row0 + 16]
        if lane0:
            out = pltpu.roll(out, 128 - lane0, 1)
        for f in (1, 2):
            piece = pltpu.roll(ends[ref][f, row0:row0 + 16], (128 - lane0 + 16 * f) % 128, 1)
            out = jnp.where(lane < 16 * f, out, piece)
        corner_out[k] = out
    pl.semaphore_wait(barrier, 8)
    sends = []
    pieces = [
        (top, south), (bottom, north),
        (side_out.at[0], sides.at[0]), (side_out.at[1], sides.at[1]),
        (corner_out.at[0], corners.at[3]), (corner_out.at[1], corners.at[2]),
        (corner_out.at[2], corners.at[1]), (corner_out.at[3], corners.at[0]),
    ]
    for k, (src, dst) in enumerate(pieces):
        sends.append(pltpu.make_async_remote_copy(
            src_ref=src, dst_ref=dst, send_sem=send.at[k], recv_sem=recv.at[k],
            device_id=ids[k], device_id_type=pl.DeviceIdType.MESH))
    for k in (4, 5, 6, 7, 2, 3, 0, 1):
        sends[k].start()
    for one in sends:
        one.wait()


def exchange(x, rows_n, cols_n):
    f32 = jnp.float32
    inside = pl.BlockSpec(memory_space=pltpu.VMEM)
    return pl.pallas_call(
        functools.partial(exchange_kernel, rows_n, cols_n),
        out_shape=(
            jax.ShapeDtypeStruct((3, 72, 128), f32),
            jax.ShapeDtypeStruct((3, 72, 128), f32),
            jax.ShapeDtypeStruct((2, 32, 128), f32),
            jax.ShapeDtypeStruct((4, 16, 128), f32),
        ),
        in_specs=[inside],
        out_specs=(inside,) * 4,
        scratch_shapes=[
            VMEM((3, 72, 128), f32),
            VMEM((3, 72, 128), f32),
            VMEM((3, ROWS, 128), f32),
            VMEM((3, ROWS, 128), f32),
            VMEM((2, 32, 128), f32),
            VMEM((4, 16, 128), f32),
            pltpu.SemaphoreType.DMA((8,)),
            pltpu.SemaphoreType.DMA((8,)),
        ],
        compiler_params=pltpu.CompilerParams(collective_id=0, has_side_effects=True, vmem_limit_bytes=8 * 1024 * 1024),
    )(x)


def cut_of(q, r):
    if 0 <= r < STRIP:
        return 0, pl.ds((q + FRONT) * PITCH + r, 8, stride=PITCH)
    return 1, pl.ds((q + FRONT) * RIM + (r > 0), 8, stride=RIM)


def take(ref, q, r):
    which, cut = cut_of(q, r)
    return ref[which][cut, :]


def put(ref, q, r, value):
    which, cut = cut_of(q, r)
    ref[which][cut, :] = value


def slopes(state, q0, act):
    e_ref, u_ref, v_ref = state

    def load(r):
        e, u, v = take(e_ref, q0, r), take(u_ref, q0, r), take(v_ref, q0, r)
        return e, u, v, (e + REST) * u

    below, here = load(-1), load(0)
    for r in range(STRIP):
        above = load(r + 1)
        e, u, v, _ = here
        de, du, dv, dw = (a - b for a, b in zip(above, below))
        east, west = ((take(e_ref, q, r), take(v_ref, q, r)) for q in (q0 + 1, q0 - 1))
        ye, yv = east[0] - west[0], east[1] - west[1]
        yu = take(u_ref, q0 + 1, r) - take(u_ref, q0 - 1, r)
        ge = dw + ((east[0] + REST) * east[1] - (west[0] + REST) * west[1])
        gu = (u * du + v * (yu - TURN)) + de
        gv = (u * (dv + TURN) + v * yv) + ye
        act(r, (e, u, v), (ge, gu, gv))
        below, here = here, above


def edges(refs, q0):
    rows = [(ref, pltpu.roll(take(ref, q0, STRIP - 1), TILES, 1), pltpu.roll(take(ref, q0, 0), 128 - TILES, 1)) for ref in refs]

    def store():
        for ref, low, high in rows:
            put(ref, q0, -1, low)
            put(ref, q0, STRIP, high)

    return store


def sweep(first, blocks, work, late, unroll):
    trips, rest = divmod(blocks, unroll)

    def trip(start, count, before):
        stores = [late(start + 8 * (k - before)) for k in range(before)]
        for k in range(count):
            work(start + 8 * k)
        for store in stores:
            store()

    trip(first, unroll, 0)

    def step(i, carry):
        trip(first + 8 * unroll * i, unroll, unroll)
        return carry

    lax.fori_loop(1, trips, step, 0)
    last = first + 8 * unroll * trips
    if rest:
        trip(last, rest, unroll)
        left = [last + 8 * k for k in range(rest)]
    else:
        left = [last + 8 * (k - unroll) for k in range(unroll)]

    def finish():
        for store in [late(q) for q in left]:
            store()

    return finish


def window_kernel(x, north, south, sides, corners, out, turned, beside, final, out_sems, *state):
    level = lax.axis_index("level")
    fields, rims = list(state[:15]), list(state[15:])
    pe, pu, pv, qe, qu, qv, ce, cu, cv = zip(fields[:9], rims)
    de, du, dv, fe, fu, fv = ((one,) for one in fields[9:])

    lane = lax.broadcasted_iota(jnp.int32, (16, 128), 1)
    for f in range(3):
        turned[f, 0:9] = sides[0, 9 * f:9 * f + 9]
        turned[f, 119:128] = sides[1, 9 * f:9 * f + 9]
        beside[f, 16:144] = jnp.transpose(turned[f])
        for k, place in ((0, 0), (2, 144)):
            west, east = pltpu.roll(corners[k], 112 - 16 * f, 1), corners[k + 1]
            if f:
                east = pltpu.roll(east, 128 - 16 * f, 1)
            beside[f, place:place + 16] = jnp.where(lane < 64, east, west)

    def tile_row(f, i):
        if i == -9:
            return north[f, 64:72]
        if i == ROWS + 8:
            return south[f, 64:72]
        if i < 0:
            return north[f, pl.ds(i + 8, TILES, stride=8), :]
        if i >= ROWS:
            return south[f, pl.ds(i - ROWS, TILES, stride=8), :]
        return x[f, pl.ds((i // 8) * 64 + i % 8, TILES, stride=8), :]

    strip_of = lax.broadcasted_iota(jnp.int32, (8, 128), 1) % TILES
    for f, ref in enumerate((pe, pu, pv)):
        outer = []
        for start in (-1, 7):
            block = [beside[f, pl.ds(16 + STRIP * s - 8 + start, 8), :] for s in range(STRIPS)]
            outer.append(jnp.transpose(jnp.concatenate(block, axis=0)) * SCALES[f])
        for r in range(-1, STRIP + 1):
            here = jnp.concatenate([tile_row(f, s * STRIP + r - 8) for s in range(STRIPS)], axis=0)
            here = jnp.transpose(here) * SCALES[f]
            for k in range(16):
                put(ref, 8 * k, r, here[8 * k:8 * k + 8])
            at = r + 1
            far = outer[at // 8]
            at %= 8
            for q in (-16, -8, 128, 136):
                k = q % 128
                toward, mine = (1, 0) if q < 0 else (127, TILES - 1)
                inner = pltpu.roll(here[k:k + 8], toward, 1)
                given = far[k:k + 8]
                if mine != at:
                    given = pltpu.roll(given, (mine - at) % 128, 1)
                put(ref, q, r, jnp.where(strip_of == mine, given, inner))

    def keep(refs, q, r, values):
        for ref, value in zip(refs, values):
            put(ref, q, r, value)

    a_state, b_state = (pe, pu, pv), (qe, qu, qv)
    c_state, d_states = (ce, cu, cv), ((de, du, dv), (fe, fu, fv))
    nothing = lambda q: lambda: None

    def predict(now, then, m, with_c):
        def work(q0):
            def act(r, own, change):
                new = tuple(p - g for p, g in zip(own, change))
                keep(then, q0, r, new)
                if with_c and m == 0:
                    keep(d_states[1], q0, r, tuple(p - 0.5 * g for p, g in zip(own, change)))
                elif with_c:
                    mid = tuple(take(ref, q0, r) - 0.5 * g for ref, g in zip(d_states[m % 2], change))
                    keep(c_state, q0, r, mid)

            slopes(now, q0, act)

        def late(q0):
            return edges(c_state + then if with_c and m else then, q0)

        reach = STEPS - m
        return sweep(-reach, (128 + 2 * reach + 7) // 8, work, late, 2)

    def correct(m):
        def work(q0):
            def act(r, own, change):
                keep(d_states[(m + 1) % 2], q0, r, tuple(take(ref, q0, r) - g for ref, g in zip(d_states[m % 2], change)))

            slopes(c_state, q0, act)

        reach = STEPS - 1 - m
        return sweep(-reach, (128 + 2 * reach + 7) // 8, work, nothing, 2)

    def last():
        def work(q0):
            def act(r, own, change):
                keep(c_state, q0, r, tuple(take(ref, q0, r) - 0.5 * g for ref, g in zip(d_states[0], change)))

            slopes(a_state, q0, act)

        sweep(0, 16, work, nothing, 2)

    def emit(refs):
        done = []
        for f, ref in enumerate(refs):
            for r in range(STRIP):
                block = jnp.concatenate([take(ref, 8 * k, r) for k in range(16)], axis=0)
                block = jnp.transpose(block) * (1.0 / SCALES[f])
                for s in range(STRIPS):
                    i = s * STRIP + r - 8
                    if 0 <= i < ROWS:
                        final[f, pl.ds((i // 8) * 64 + i % 8, TILES, stride=8), :] = block[8 * s:8 * s + 8]
            done.append(pltpu.make_async_copy(final.at[f], out.at[0, f], out_sems.at[f]))
            done[-1].start()
        for copy in done:
            copy.wait()

    @pl.when(level == 0)
    def _():
        for m in range(STEPS):
            now, then = (a_state, b_state) if m % 2 == 0 else (b_state, a_state)
            predict(now, then, m, False)()
        emit(a_state)

    @pl.when(level == 1)
    def _():
        for m in range(STEPS):
            now, then = (a_state, b_state) if m % 2 == 0 else (b_state, a_state)
            predict(now, then, m, True)()
            if m:
                correct(m)
        last()
        emit(c_state)


def window(x, *halo):
    f32 = jnp.float32
    inside = pl.BlockSpec(memory_space=pltpu.VMEM)
    return pl.pallas_call(
        window_kernel,
        out_shape=jax.ShapeDtypeStruct((1, 3, ROWS * TILES, 128), f32),
        in_specs=[inside] * 5,
        out_specs=pl.BlockSpec(memory_space=pltpu.HBM),
        scratch_shapes=[
            VMEM((3, 128, 128), f32),
            VMEM((3, 160, 128), f32),
            VMEM((3, ROWS * TILES, 128), f32),
            pltpu.SemaphoreType.DMA((3,)),
        ] + [VMEM((WORDS, 128), f32) for _ in range(15)] + [VMEM((SPAN * RIM, 128), f32) for _ in range(9)],
        compiler_params=pltpu.CompilerParams(vmem_limit_bytes=32 * 1024 * 1024),
    )(x, *halo)


def solution(mesh):
    rows_n, cols_n = mesh.shape["row"], mesh.shape["col"]

    def body(x):
        words = x.reshape(3, ROWS // 8, 8, TILES, 128).transpose(0, 1, 3, 2, 4).reshape(3, ROWS * TILES, 128)
        done = window(words, *exchange(words, rows_n, cols_n))
        return done.reshape(1, 3, ROWS // 8, TILES, 8, 128).transpose(0, 1, 2, 4, 3, 5).reshape(1, 3, ROWS, COLS)

    return jax.shard_map(
        body,
        mesh=mesh,
        in_specs=(P(None, "row", "col"),),
        out_specs=P("level", None, "row", "col"),
        check_vma=False,
    )
```

```python
import functools

import jax
import jax.numpy as jnp
from jax import lax
from jax.experimental import pallas as pl
from jax.experimental.pallas import tpu as pltpu
from jax.sharding import PartitionSpec as P

STEPS = 8
TIME_STEP = 0.1
GRAVITY = 1.0
ROTATION = 0.2

HALF = 0.5 * TIME_STEP
SCALES = (HALF * HALF * GRAVITY, HALF, HALF)
REST = HALF * HALF * GRAVITY
TURN = TIME_STEP * ROTATION

ROWS = 128
COLS = 1024
TILES = COLS // 128
STRIP = 9
STRIPS = 16
PITCH = 9
RIM = 3
FRONT = 16
SPAN = 128 + 2 * FRONT
WORDS = SPAN * PITCH
VMEM = pltpu.VMEM


def meet(places):
    barrier = pltpu.get_barrier_semaphore()
    for where in places:
        pl.semaphore_signal(barrier, inc=1, device_id=where, device_id_type=pl.DeviceIdType.MESH)
    return barrier


def remote(k, src, dst, where, send, recv):
    return pltpu.make_async_remote_copy(
        src_ref=src, dst_ref=dst, send_sem=send.at[k], recv_sem=recv.at[k],
        device_id=where, device_id_type=pl.DeviceIdType.MESH)


def around(axis, count):
    me = lax.axis_index(axis)
    return lax.rem(me + count - 1, count), lax.rem(me + 1, count)


def rows_kernel(rows_n, x, north, south, top, bottom, send, recv):
    up, down = around("row", rows_n)
    barrier = meet([{"row": up}, {"row": down}])
    for f in range(3):
        top[f, 0:64] = x[f, 0:64]
        bottom[f, 0:64] = x[f, 8 * ROWS - 64:8 * ROWS]
        top[f, 64:72] = x[f, pl.ds(64, TILES, stride=8), :]
        bottom[f, 64:72] = x[f, pl.ds(8 * ROWS - 128 + 7, TILES, stride=8), :]
        top[f, 72:80] = jnp.zeros((8, 128), jnp.float32)
        bottom[f, 72:80] = jnp.zeros((8, 128), jnp.float32)
    pl.semaphore_wait(barrier, 2)
    copies = [remote(0, top, south, {"row": up}, send, recv), remote(1, bottom, north, {"row": down}, send, recv)]
    for copy in copies:
        copy.start()
    for copy in copies:
        copy.wait()


def swap_rows(x, rows_n):
    f32 = jnp.float32
    inside = pl.BlockSpec(memory_space=pltpu.VMEM)
    return pl.pallas_call(
        functools.partial(rows_kernel, rows_n),
        out_shape=(jax.ShapeDtypeStruct((3, 80, 128), f32), jax.ShapeDtypeStruct((3, 80, 128), f32)),
        in_specs=[inside],
        out_specs=(inside,) * 2,
        scratch_shapes=[
            VMEM((3, 80, 128), f32),
            VMEM((3, 80, 128), f32),
            pltpu.SemaphoreType.DMA((2,)),
            pltpu.SemaphoreType.DMA((2,)),
        ],
        compiler_params=pltpu.CompilerParams(collective_id=0, has_side_effects=True, vmem_limit_bytes=4 * 1024 * 1024),
    )(x)


def cut_of(q, r):
    if 0 <= r < STRIP:
        return 0, pl.ds((q + FRONT) * PITCH + r, 8, stride=PITCH)
    return 1, pl.ds((q + FRONT) * RIM + (r > 0), 8, stride=RIM)


def take(ref, q, r):
    which, cut = cut_of(q, r)
    return ref[which][cut, :]


def put(ref, q, r, value):
    which, cut = cut_of(q, r)
    ref[which][cut, :] = value


def slopes(state, q0, act):
    e_ref, u_ref, v_ref = state

    def load(r):
        e, u, v = take(e_ref, q0, r), take(u_ref, q0, r), take(v_ref, q0, r)
        return e, u, v, (e + REST) * u

    below, here = load(-1), load(0)
    for r in range(STRIP):
        above = load(r + 1)
        e, u, v, _ = here
        de, du, dv, dw = (a - b for a, b in zip(above, below))
        east, west = ((take(e_ref, q, r), take(v_ref, q, r)) for q in (q0 + 1, q0 - 1))
        ye, yv = east[0] - west[0], east[1] - west[1]
        yu = take(u_ref, q0 + 1, r) - take(u_ref, q0 - 1, r)
        ge = dw + ((east[0] + REST) * east[1] - (west[0] + REST) * west[1])
        gu = (u * du + v * (yu - TURN)) + de
        gv = (u * (dv + TURN) + v * yv) + ye
        act(r, (e, u, v), (ge, gu, gv))
        below, here = here, above


def edges(refs, q0):
    rows = [(ref, pltpu.roll(take(ref, q0, STRIP - 1), TILES, 1), pltpu.roll(take(ref, q0, 0), 128 - TILES, 1)) for ref in refs]

    def store():
        for ref, low, high in rows:
            put(ref, q0, -1, low)
            put(ref, q0, STRIP, high)

    return store


def sweep(first, blocks, work, late, unroll):
    trips, rest = divmod(blocks, unroll)

    def trip(start, count, before):
        stores = [late(start + 8 * (k - before)) for k in range(before)]
        for k in range(count):
            work(start + 8 * k)
        for store in stores:
            store()

    trip(first, unroll, 0)

    def step(i, carry):
        trip(first + 8 * unroll * i, unroll, unroll)
        return carry

    lax.fori_loop(1, trips, step, 0)
    last = first + 8 * unroll * trips
    if rest:
        trip(last, rest, unroll)
        left = [last + 8 * k for k in range(rest)]
    else:
        left = [last + 8 * (k - unroll) for k in range(unroll)]

    def finish():
        for store in [late(q) for q in left]:
            store()

    return finish


def run(level, a_state, b_state, c_state, d_states, out_state, origin, width, early=None):
    nothing = lambda q: lambda: None

    def keep(refs, q, r, values):
        for ref, value in zip(refs, values):
            put(ref, q, r, value)

    def blocks(reach):
        return origin - reach, (width + 2 * reach + 7) // 8

    def predict(now, then, m, with_c):
        def work(q0):
            def act(r, own, change):
                keep(then, q0, r, tuple(p - g for p, g in zip(own, change)))
                if with_c and m == 0:
                    keep(d_states[1], q0, r, tuple(p - 0.5 * g for p, g in zip(own, change)))
                elif with_c:
                    keep(c_state, q0, r, tuple(take(ref, q0, r) - 0.5 * g for ref, g in zip(d_states[m % 2], change)))

            slopes(now, q0, act)

        def late(q0):
            return edges(c_state + then if with_c and m else then, q0)

        end = m == STEPS - 1 and not with_c
        return sweep(*blocks(STEPS - m), work, nothing if end else late, 2)

    def correct(m):
        def work(q0):
            def act(r, own, change):
                keep(d_states[(m + 1) % 2], q0, r, tuple(take(ref, q0, r) - g for ref, g in zip(d_states[m % 2], change)))

            slopes(c_state, q0, act)

        return sweep(*blocks(STEPS - 1 - m), work, nothing, 2)

    def last():
        def work(q0):
            def act(r, own, change):
                keep(out_state, q0, r, tuple(take(ref, q0, r) - 0.5 * g for ref, g in zip(d_states[0], change)))

            slopes(a_state, q0, act)

        sweep(*blocks(0), work, nothing, 2)

    def steps(with_c):
        for m in range(STEPS):
            if early is not None:
                early(with_c, m)
            now, then = (a_state, b_state) if m % 2 == 0 else (b_state, a_state)
            if m == STEPS - 1 and not with_c:
                then = out_state
            predict(now, then, m, with_c)()
            if with_c and m:
                correct(m)
        if with_c:
            last()
        if early is not None:
            early(with_c, STEPS)

    @pl.when(level == 0)
    def _():
        steps(False)

    @pl.when(level == 1)
    def _():
        steps(True)


def split_state(state):
    fields, rims = list(state[:15]), list(state[15:])
    pairs = list(zip(fields[:9], rims))
    single = [(one,) for one in fields[9:]]
    return tuple(pairs[:3]), tuple(pairs[3:6]), tuple(pairs[6:9]), (tuple(single[:3]), tuple(single[3:6]))


def state_scratch(span):
    f32 = jnp.float32
    return [VMEM((span * PITCH, 128), f32) for _ in range(15)] + [VMEM((span * RIM, 128), f32) for _ in range(9)]


SEND_AHEAD = ((STEPS, 4, 2, 0), (5, 2, 1, 0))


def main_kernel(rows_n, cols_n, x, north, south, sides, corners, oe, ou, ov,
                side_out, corner_out, send, recv, *state):
    level = lax.axis_index("level")
    up, down = around("row", rows_n)
    west, east = around("col", cols_n)
    ids = [{"col": west}, {"col": east}] + [{"row": r, "col": c} for r in (up, down) for c in (west, east)]
    barrier = meet(ids)
    group = lax.rem(lax.axis_index("col"), len(SEND_AHEAD[0]))

    lane = lax.broadcasted_iota(jnp.int32, (16, 128), 1)
    view = x.reshape(3, ROWS // 8, 8 * TILES, 128)

    def column(f, c, t0, t1):
        return view[f, t0:t1, 8 * c:8 * c + 8, :].reshape(8 * (t1 - t0), 128)

    for f in range(3):
        side_out[0, 9 * f:9 * f + 9] = jnp.transpose(column(f, 0, 0, 16))[0:9]
        side_out[1, 9 * f:9 * f + 9] = jnp.transpose(column(f, TILES - 1, 0, 16))[119:128]
    for k, (c, t, lane0) in enumerate(((0, 0, 0), (TILES - 1, 0, 112), (0, 14, 0), (TILES - 1, 14, 112))):
        out = column(0, c, t, t + 2)
        if lane0:
            out = pltpu.roll(out, 128 - lane0, 1)
        for f in (1, 2):
            piece = pltpu.roll(column(f, c, t, t + 2), (128 - lane0 + 16 * f) % 128, 1)
            out = jnp.where(lane < 16 * f, out, piece)
        corner_out[k] = out
    pieces = [(side_out.at[0], sides.at[0]), (side_out.at[1], sides.at[1])]
    pieces += [(corner_out.at[k], corners.at[3 - k]) for k in range(4)]
    copies = [remote(k, *piece, where, send, recv) for k, (piece, where) in enumerate(zip(pieces, ids))]

    def early(with_c, m):
        turns = SEND_AHEAD[int(with_c)]
        for k, turn in enumerate(turns):
            if turn == m:
                @pl.when(group == k)
                def _():
                    pl.semaphore_wait(barrier, 6)
                    for copy in copies:
                        copy.start()

    a_state, b_state, c_state, d_states = split_state(state)

    def tile_row(f, i):
        if i == -9:
            return north[f, 64:72]
        if i == ROWS + 8:
            return south[f, 64:72]
        if i < 0:
            return north[f, pl.ds(i + 8, TILES, stride=8), :]
        if i >= ROWS:
            return south[f, pl.ds(i - ROWS, TILES, stride=8), :]
        return x[f, pl.ds((i // 8) * 64 + i % 8, TILES, stride=8), :]

    for f, ref in enumerate(a_state):
        for r in range(-1, STRIP + 1):
            here = jnp.concatenate([tile_row(f, s * STRIP + r - 8) for s in range(STRIPS)], axis=0)
            here = jnp.transpose(here) * SCALES[f]
            for k in range(16):
                put(ref, 8 * k, r, here[8 * k:8 * k + 8])
            for q in (-16, -8, 128, 136):
                k = q % 128
                put(ref, q, r, pltpu.roll(here[k:k + 8], 1 if q < 0 else 127, 1))

    run(level, a_state, b_state, c_state, d_states, ((oe,), (ou,), (ov,)), 0, 128, early)
    for copy in copies:
        copy.wait()


def main(x, north, south, rows_n, cols_n):
    f32 = jnp.float32
    inside = pl.BlockSpec(memory_space=pltpu.VMEM)
    return pl.pallas_call(
        functools.partial(main_kernel, rows_n, cols_n),
        out_shape=(
            jax.ShapeDtypeStruct((2, 32, 128), f32),
            jax.ShapeDtypeStruct((4, 16, 128), f32),
        ) + (jax.ShapeDtypeStruct((WORDS, 128), f32),) * 3,
        in_specs=[inside] * 3,
        out_specs=(inside,) * 5,
        scratch_shapes=[
            VMEM((2, 32, 128), f32),
            VMEM((4, 16, 128), f32),
            pltpu.SemaphoreType.DMA((6,)),
            pltpu.SemaphoreType.DMA((6,)),
        ] + state_scratch(SPAN),
        compiler_params=pltpu.CompilerParams(collective_id=1, has_side_effects=True, vmem_limit_bytes=32 * 1024 * 1024),
    )(x, north, south)


BAND = 9
BAND_SPAN = 64


def band_kernel(x, north, south, sides, corners, oe, ou, ov, out, turned, beside, band, final, out_sems, be, bu, bv, *state):
    level = lax.axis_index("level")
    a_state, b_state, c_state, d_states = split_state(state)
    lane16 = lax.broadcasted_iota(jnp.int32, (16, 128), 1)
    lane8 = lax.broadcasted_iota(jnp.int32, (8, 128), 1)

    for f in range(3):
        turned[f, 0:9] = sides[0, 9 * f:9 * f + 9]
        turned[f, 119:128] = sides[1, 9 * f:9 * f + 9]
        beside[f, 16:144] = jnp.transpose(turned[f])
        for k, place in ((0, 0), (2, 144)):
            west, east = pltpu.roll(corners[k], 112 - 16 * f, 1), corners[k + 1]
            if f:
                east = pltpu.roll(east, 128 - 16 * f, 1)
            beside[f, place:place + 16] = jnp.where(lane16 < 64, east, west)

    def own(f, c, t):
        if t == -2:
            return north[f, 57 + c:65 + c]
        if t == -1:
            return north[f, 8 * c:8 * c + 8]
        if t == 16:
            return south[f, 8 * c:8 * c + 8]
        if t == 17:
            return south[f, 64 + c:72 + c]
        return x[f, 64 * t + 8 * c:64 * t + 8 * c + 8]

    for f in range(3):
        for t in range(-2, 18):
            row = 8 * (t + 2)
            outer = beside[f, row:row + 8]
            low = pltpu.roll(jnp.where(lane8 >= 64, outer, own(f, 0, t)), 9, 1)
            high = pltpu.roll(jnp.where(lane8 < 64, outer, own(f, TILES - 1, t)), 82, 1)
            band[f, row:row + 8] = jnp.where(lane8 < 64, low, high)

    strip_of = lane8 % TILES
    for f, ref in enumerate(a_state):
        blocks = []
        for start in (-1, 7):
            block = [band[f, pl.ds(16 + STRIP * s - 8 + start, 8), :] for s in range(STRIPS)]
            blocks.append(jnp.transpose(jnp.concatenate(block, axis=0)) * SCALES[f])
        for r in range(-1, STRIP + 1):
            far, at = blocks[(r + 1) // 8], (r + 1) % 8
            for k in range(4):
                low, high = far[8 * k:8 * k + 8], far[64 + 8 * k:72 + 8 * k]
                if at:
                    low = pltpu.roll(low, 128 - at, 1)
                if at != TILES - 1:
                    high = pltpu.roll(high, TILES - 1 - at, 1)
                put(ref, 8 * k, r, jnp.where(strip_of == TILES - 1, high, low))

    b_out = ((be,), (bu,), (bv,))
    run(level, a_state, b_state, c_state, d_states, b_out, BAND, BAND)

    word_of = lax.broadcasted_iota(jnp.int32, (8, 128), 0)
    first, end = strip_of == 0, strip_of == TILES - 1
    done = []
    for f, (ref, fix) in enumerate(zip((oe, ou, ov), b_out)):
        for r in range(STRIP):
            block = [take((ref,), 8 * k, r) for k in range(16)]
            block[0] = jnp.where(first, take(fix, 9, r), block[0])
            block[1] = jnp.where(first & (word_of == 0), take(fix, 17, r), block[1])
            block[14] = jnp.where(end & (word_of == 7), take(fix, 2, r), block[14])
            block[15] = jnp.where(end, take(fix, 10, r), block[15])
            block = jnp.transpose(jnp.concatenate(block, axis=0)) * (1.0 / SCALES[f])
            for s in range(STRIPS):
                i = s * STRIP + r - 8
                if 0 <= i < ROWS:
                    final[f, pl.ds((i // 8) * 64 + i % 8, TILES, stride=8), :] = block[8 * s:8 * s + 8]
        done.append(pltpu.make_async_copy(final.at[f], out.at[0, f], out_sems.at[f]))
        done[-1].start()
    for copy in done:
        copy.wait()


def bands(x, *rest):
    f32 = jnp.float32
    inside = pl.BlockSpec(memory_space=pltpu.VMEM)
    return pl.pallas_call(
        band_kernel,
        out_shape=jax.ShapeDtypeStruct((1, 3, ROWS * TILES, 128), f32),
        in_specs=[inside] * 8,
        out_specs=pl.BlockSpec(memory_space=pltpu.HBM),
        scratch_shapes=[
            VMEM((3, 128, 128), f32),
            VMEM((3, 160, 128), f32),
            VMEM((3, 160, 128), f32),
            VMEM((3, ROWS * TILES, 128), f32),
            pltpu.SemaphoreType.DMA((3,)),
        ] + [VMEM((BAND_SPAN * PITCH, 128), f32) for _ in range(3)] + state_scratch(BAND_SPAN),
        compiler_params=pltpu.CompilerParams(vmem_limit_bytes=16 * 1024 * 1024),
    )(x, *rest)


def solution(mesh):
    rows_n, cols_n = mesh.shape["row"], mesh.shape["col"]

    def body(x):
        words = x.reshape(3, ROWS // 8, 8, TILES, 128).transpose(0, 1, 3, 2, 4).reshape(3, ROWS * TILES, 128)
        north, south = swap_rows(words, rows_n)
        done = bands(words, north, south, *main(words, north, south, rows_n, cols_n))
        return done.reshape(1, 3, ROWS // 8, TILES, 8, 128).transpose(0, 1, 2, 4, 3, 5).reshape(1, 3, ROWS, COLS)

    return jax.shard_map(
        body,
        mesh=mesh,
        in_specs=(P(None, "row", "col"),),
        out_specs=P("level", None, "row", "col"),
        check_vma=False,
    )
```

```python
import functools

import jax
import jax.numpy as jnp
from jax import lax
from jax.experimental import pallas as pl
from jax.experimental.pallas import tpu as pltpu
from jax.sharding import PartitionSpec as P

STEPS = 8
TIME_STEP = 0.1
GRAVITY = 1.0
ROTATION = 0.2

HALF = 0.5 * TIME_STEP
SCALES = (HALF * HALF * GRAVITY, HALF, HALF)
REST = HALF * HALF * GRAVITY
TURN = TIME_STEP * ROTATION

ROWS = 128
COLS = 1024
TILES = COLS // 128
STRIP = 9
STRIPS = 16
PITCH = 9
RIM = 3
FRONT = 16
SPAN = 128 + 2 * FRONT
WORDS = SPAN * PITCH
VMEM = pltpu.VMEM


def meet(places):
    barrier = pltpu.get_barrier_semaphore()
    for where in places:
        pl.semaphore_signal(barrier, inc=1, device_id=where, device_id_type=pl.DeviceIdType.MESH)
    return barrier


def remote(k, src, dst, where, send, recv):
    return pltpu.make_async_remote_copy(
        src_ref=src, dst_ref=dst, send_sem=send.at[k], recv_sem=recv.at[k],
        device_id=where, device_id_type=pl.DeviceIdType.MESH)


def around(axis, count):
    me = lax.axis_index(axis)
    return lax.rem(me + count - 1, count), lax.rem(me + 1, count)


def rows_kernel(rows_n, x, north, south, top, bottom, send, recv):
    up, down = around("row", rows_n)
    barrier = meet([{"row": up}, {"row": down}])
    for f in range(3):
        top[f, 0:64] = x[f, 0:64]
        bottom[f, 0:64] = x[f, 8 * ROWS - 64:8 * ROWS]
        top[f, 64:72] = x[f, pl.ds(64, TILES, stride=8), :]
        bottom[f, 64:72] = x[f, pl.ds(8 * ROWS - 128 + 7, TILES, stride=8), :]
        top[f, 72:80] = jnp.zeros((8, 128), jnp.float32)
        bottom[f, 72:80] = jnp.zeros((8, 128), jnp.float32)
    pl.semaphore_wait(barrier, 2)
    copies = [remote(0, top, south, {"row": up}, send, recv), remote(1, bottom, north, {"row": down}, send, recv)]
    for copy in copies:
        copy.start()
    for copy in copies:
        copy.wait()


def swap_rows(x, rows_n):
    f32 = jnp.float32
    inside = pl.BlockSpec(memory_space=pltpu.VMEM)
    return pl.pallas_call(
        functools.partial(rows_kernel, rows_n),
        out_shape=(jax.ShapeDtypeStruct((3, 80, 128), f32), jax.ShapeDtypeStruct((3, 80, 128), f32)),
        in_specs=[inside],
        out_specs=(inside,) * 2,
        scratch_shapes=[
            VMEM((3, 80, 128), f32),
            VMEM((3, 80, 128), f32),
            pltpu.SemaphoreType.DMA((2,)),
            pltpu.SemaphoreType.DMA((2,)),
        ],
        compiler_params=pltpu.CompilerParams(collective_id=0, has_side_effects=True, vmem_limit_bytes=4 * 1024 * 1024),
    )(x)


def cut_of(q, r):
    if 0 <= r < STRIP:
        return 0, pl.ds((q + FRONT) * PITCH + r, 8, stride=PITCH)
    return 1, pl.ds((q + FRONT) * RIM + (r > 0), 8, stride=RIM)


def take(ref, q, r):
    which, cut = cut_of(q, r)
    return ref[which][cut, :]


def put(ref, q, r, value):
    which, cut = cut_of(q, r)
    ref[which][cut, :] = value


def slopes(state, q0, act):
    e_ref, u_ref, v_ref = state

    def load(r):
        e, u, v = take(e_ref, q0, r), take(u_ref, q0, r), take(v_ref, q0, r)
        return e, u, v, (e + REST) * u

    below, here = load(-1), load(0)
    for r in range(STRIP):
        above = load(r + 1)
        e, u, v, _ = here
        de, du, dv, dw = (a - b for a, b in zip(above, below))
        east, west = ((take(e_ref, q, r), take(v_ref, q, r)) for q in (q0 + 1, q0 - 1))
        ye, yv = east[0] - west[0], east[1] - west[1]
        yu = take(u_ref, q0 + 1, r) - take(u_ref, q0 - 1, r)
        ge = dw + ((east[0] + REST) * east[1] - (west[0] + REST) * west[1])
        gu = (u * du + v * (yu - TURN)) + de
        gv = (u * (dv + TURN) + v * yv) + ye
        act(r, (e, u, v), (ge, gu, gv))
        below, here = here, above


def edges(refs, q0):
    rows = [(ref, pltpu.roll(take(ref, q0, STRIP - 1), TILES, 1), pltpu.roll(take(ref, q0, 0), 128 - TILES, 1)) for ref in refs]

    def store():
        for ref, low, high in rows:
            put(ref, q0, -1, low)
            put(ref, q0, STRIP, high)

    return store


def sweep(first, blocks, work, late, unroll):
    trips, rest = divmod(blocks, unroll)

    def trip(start, count, before):
        stores = [late(start + 8 * (k - before)) for k in range(before)]
        for k in range(count):
            work(start + 8 * k)
        for store in stores:
            store()

    trip(first, unroll, 0)

    def step(i, carry):
        trip(first + 8 * unroll * i, unroll, unroll)
        return carry

    lax.fori_loop(1, trips, step, 0)
    last = first + 8 * unroll * trips
    if rest:
        trip(last, rest, unroll)
        left = [last + 8 * k for k in range(rest)]
    else:
        left = [last + 8 * (k - unroll) for k in range(unroll)]

    def finish():
        for store in [late(q) for q in left]:
            store()

    return finish


def run(level, a_state, b_state, c_state, d_states, out_state, origin, width, early=None):
    nothing = lambda q: lambda: None

    def keep(refs, q, r, values):
        for ref, value in zip(refs, values):
            put(ref, q, r, value)

    def blocks(reach):
        return origin - reach, (width + 2 * reach + 7) // 8

    def predict(now, then, m, with_c):
        def work(q0):
            def act(r, own, change):
                keep(then, q0, r, tuple(p - g for p, g in zip(own, change)))
                if with_c and m == 0:
                    keep(d_states[1], q0, r, tuple(p - 0.5 * g for p, g in zip(own, change)))
                elif with_c:
                    keep(c_state, q0, r, tuple(take(ref, q0, r) - 0.5 * g for ref, g in zip(d_states[m % 2], change)))

            slopes(now, q0, act)

        def late(q0):
            return edges(c_state + then if with_c and m else then, q0)

        end = m == STEPS - 1 and not with_c
        return sweep(*blocks(STEPS - m), work, nothing if end else late, 2)

    def correct(m):
        def work(q0):
            def act(r, own, change):
                keep(d_states[(m + 1) % 2], q0, r, tuple(take(ref, q0, r) - g for ref, g in zip(d_states[m % 2], change)))

            slopes(c_state, q0, act)

        return sweep(*blocks(STEPS - 1 - m), work, nothing, 2)

    def last():
        def work(q0):
            def act(r, own, change):
                keep(out_state, q0, r, tuple(take(ref, q0, r) - 0.5 * g for ref, g in zip(d_states[0], change)))

            slopes(a_state, q0, act)

        sweep(*blocks(0), work, nothing, 2)

    def steps(with_c):
        for m in range(STEPS):
            if early is not None:
                early(with_c, m)
            now, then = (a_state, b_state) if m % 2 == 0 else (b_state, a_state)
            if m == STEPS - 1 and not with_c:
                then = out_state
            predict(now, then, m, with_c)()
            if with_c and m:
                correct(m)
        if with_c:
            last()
        if early is not None:
            early(with_c, STEPS)

    @pl.when(level == 0)
    def _():
        steps(False)

    @pl.when(level == 1)
    def _():
        steps(True)


def split_state(state):
    fields, rims = list(state[:15]), list(state[15:])
    pairs = list(zip(fields[:9], rims))
    single = [(one,) for one in fields[9:]]
    return tuple(pairs[:3]), tuple(pairs[3:6]), tuple(pairs[6:9]), (tuple(single[:3]), tuple(single[3:6]))


def state_scratch(span):
    f32 = jnp.float32
    return [VMEM((span * PITCH, 128), f32) for _ in range(15)] + [VMEM((span * RIM, 128), f32) for _ in range(9)]


SEND_AHEAD = ((STEPS, 3, 3, 0), (5, 2, 2, 0))


def own_tile(x, north, south, f, c, t):
    if t == -2:
        return north[f, 57 + c:65 + c]
    if t == -1:
        return north[f, 8 * c:8 * c + 8]
    if t == ROWS // 8:
        return south[f, 8 * c:8 * c + 8]
    if t == ROWS // 8 + 1:
        return south[f, 64 + c:72 + c]
    return x[f, 64 * t + 8 * c:64 * t + 8 * c + 8]


def main_kernel(cols_n, x, north, south, sides, oe, ou, ov, side_out, send, recv, *state):
    level = lax.axis_index("level")
    west, east = around("col", cols_n)
    ids = [{"col": west}, {"col": east}]
    barrier = meet(ids)
    group = lax.rem(lax.axis_index("col"), len(SEND_AHEAD[0]))

    lane = lax.broadcasted_iota(jnp.int32, (8, 128), 1)
    view = x.reshape(3, ROWS // 8, 8 * TILES, 128)
    for k, (c, lane0) in enumerate(((0, 0), (TILES - 1, 112))):
        for f in range(3):
            whole = jnp.transpose(view[f, :, 8 * c:8 * c + 8, :].reshape(ROWS, 128))
            side_out[k, 9 * f:9 * f + 9] = whole[119:128] if k else whole[0:9]
        for j, t in enumerate((-2, -1, 16, 17)):
            out = own_tile(x, north, south, 0, c, t)
            if lane0:
                out = pltpu.roll(out, 128 - lane0, 1)
            for f in (1, 2):
                piece = pltpu.roll(own_tile(x, north, south, f, c, t), (128 - lane0 + 16 * f) % 128, 1)
                out = jnp.where(lane < 16 * f, out, piece)
            side_out[k, 32 + 8 * j:40 + 8 * j] = out
    copies = [remote(k, side_out.at[k], sides.at[k], ids[k], send, recv) for k in range(2)]

    def early(with_c, m):
        turns = SEND_AHEAD[int(with_c)]
        for k, turn in enumerate(turns):
            if turn == m:
                @pl.when(group == k)
                def _():
                    pl.semaphore_wait(barrier, 2)
                    for copy in copies:
                        copy.start()

    a_state, b_state, c_state, d_states = split_state(state)

    def tile_row(f, i):
        if i == -9:
            return north[f, 64:72]
        if i == ROWS + 8:
            return south[f, 64:72]
        if i < 0:
            return north[f, pl.ds(i + 8, TILES, stride=8), :]
        if i >= ROWS:
            return south[f, pl.ds(i - ROWS, TILES, stride=8), :]
        return x[f, pl.ds((i // 8) * 64 + i % 8, TILES, stride=8), :]

    for f, ref in enumerate(a_state):
        for r in range(-1, STRIP + 1):
            here = jnp.concatenate([tile_row(f, s * STRIP + r - 8) for s in range(STRIPS)], axis=0)
            here = jnp.transpose(here) * SCALES[f]
            for k in range(16):
                put(ref, 8 * k, r, here[8 * k:8 * k + 8])
            for q in (-16, -8, 128, 136):
                k = q % 128
                put(ref, q, r, pltpu.roll(here[k:k + 8], 1 if q < 0 else 127, 1))

    run(level, a_state, b_state, c_state, d_states, ((oe,), (ou,), (ov,)), 0, 128, early)
    for copy in copies:
        copy.wait()


def main(x, north, south, cols_n):
    f32 = jnp.float32
    inside = pl.BlockSpec(memory_space=pltpu.VMEM)
    return pl.pallas_call(
        functools.partial(main_kernel, cols_n),
        out_shape=(jax.ShapeDtypeStruct((2, 64, 128), f32),) + (jax.ShapeDtypeStruct((WORDS, 128), f32),) * 3,
        in_specs=[inside] * 3,
        out_specs=(inside,) * 4,
        scratch_shapes=[
            VMEM((2, 64, 128), f32),
            pltpu.SemaphoreType.DMA((2,)),
            pltpu.SemaphoreType.DMA((2,)),
        ] + state_scratch(SPAN),
        compiler_params=pltpu.CompilerParams(collective_id=1, has_side_effects=True, vmem_limit_bytes=32 * 1024 * 1024),
    )(x, north, south)


BAND = 9
BAND_SPAN = 64


def band_kernel(x, north, south, sides, oe, ou, ov, out, turned, beside, band, final, out_sems, be, bu, bv, *state):
    level = lax.axis_index("level")
    a_state, b_state, c_state, d_states = split_state(state)
    lane16 = lax.broadcasted_iota(jnp.int32, (16, 128), 1)
    lane8 = lax.broadcasted_iota(jnp.int32, (8, 128), 1)

    for f in range(3):
        turned[f, 0:9] = sides[0, 9 * f:9 * f + 9]
        turned[f, 119:128] = sides[1, 9 * f:9 * f + 9]
        beside[f, 16:144] = jnp.transpose(turned[f])
        for k, place in ((32, 0), (48, 144)):
            west, east = pltpu.roll(sides[1, k:k + 16], 112 - 16 * f, 1), sides[0, k:k + 16]
            if f:
                east = pltpu.roll(east, 128 - 16 * f, 1)
            beside[f, place:place + 16] = jnp.where(lane16 < 64, east, west)

    for f in range(3):
        for t in range(-2, 18):
            row = 8 * (t + 2)
            outer = beside[f, row:row + 8]
            low = pltpu.roll(jnp.where(lane8 >= 64, outer, own_tile(x, north, south, f, 0, t)), 9, 1)
            high = pltpu.roll(jnp.where(lane8 < 64, outer, own_tile(x, north, south, f, TILES - 1, t)), 82, 1)
            band[f, row:row + 8] = jnp.where(lane8 < 64, low, high)

    strip_of = lane8 % TILES
    for f, ref in enumerate(a_state):
        blocks = []
        for start in (-1, 7):
            block = [band[f, pl.ds(16 + STRIP * s - 8 + start, 8), :] for s in range(STRIPS)]
            blocks.append(jnp.transpose(jnp.concatenate(block, axis=0)) * SCALES[f])
        for r in range(-1, STRIP + 1):
            far, at = blocks[(r + 1) // 8], (r + 1) % 8
            for k in range(4):
                low, high = far[8 * k:8 * k + 8], far[64 + 8 * k:72 + 8 * k]
                if at:
                    low = pltpu.roll(low, 128 - at, 1)
                if at != TILES - 1:
                    high = pltpu.roll(high, TILES - 1 - at, 1)
                put(ref, 8 * k, r, jnp.where(strip_of == TILES - 1, high, low))

    b_out = ((be,), (bu,), (bv,))
    run(level, a_state, b_state, c_state, d_states, b_out, BAND, BAND)

    word_of = lax.broadcasted_iota(jnp.int32, (8, 128), 0)
    first, end = strip_of == 0, strip_of == TILES - 1
    done = []
    for f, (ref, fix) in enumerate(zip((oe, ou, ov), b_out)):
        for r in range(STRIP):
            block = [take((ref,), 8 * k, r) for k in range(16)]
            block[0] = jnp.where(first, take(fix, 9, r), block[0])
            block[1] = jnp.where(first & (word_of == 0), take(fix, 17, r), block[1])
            block[14] = jnp.where(end & (word_of == 7), take(fix, 2, r), block[14])
            block[15] = jnp.where(end, take(fix, 10, r), block[15])
            block = jnp.transpose(jnp.concatenate(block, axis=0)) * (1.0 / SCALES[f])
            for s in range(STRIPS):
                i = s * STRIP + r - 8
                if 0 <= i < ROWS:
                    final[f, pl.ds((i // 8) * 64 + i % 8, TILES, stride=8), :] = block[8 * s:8 * s + 8]
        done.append(pltpu.make_async_copy(final.at[f], out.at[0, f], out_sems.at[f]))
        done[-1].start()
    for copy in done:
        copy.wait()


def bands(x, *rest):
    f32 = jnp.float32
    inside = pl.BlockSpec(memory_space=pltpu.VMEM)
    return pl.pallas_call(
        band_kernel,
        out_shape=jax.ShapeDtypeStruct((1, 3, ROWS * TILES, 128), f32),
        in_specs=[inside] * 7,
        out_specs=pl.BlockSpec(memory_space=pltpu.HBM),
        scratch_shapes=[
            VMEM((3, 128, 128), f32),
            VMEM((3, 160, 128), f32),
            VMEM((3, 160, 128), f32),
            VMEM((3, ROWS * TILES, 128), f32),
            pltpu.SemaphoreType.DMA((3,)),
        ] + [VMEM((BAND_SPAN * PITCH, 128), f32) for _ in range(3)] + state_scratch(BAND_SPAN),
        compiler_params=pltpu.CompilerParams(vmem_limit_bytes=16 * 1024 * 1024),
    )(x, *rest)


def solution(mesh):
    rows_n, cols_n = mesh.shape["row"], mesh.shape["col"]

    def body(x):
        words = x.reshape(3, ROWS // 8, 8, TILES, 128).transpose(0, 1, 3, 2, 4).reshape(3, ROWS * TILES, 128)
        north, south = swap_rows(words, rows_n)
        done = bands(words, north, south, *main(words, north, south, cols_n))
        return done.reshape(1, 3, ROWS // 8, TILES, 8, 128).transpose(0, 1, 2, 4, 3, 5).reshape(1, 3, ROWS, COLS)

    return jax.shard_map(
        body,
        mesh=mesh,
        in_specs=(P(None, "row", "col"),),
        out_specs=P("level", None, "row", "col"),
        check_vma=False,
    )
```

```python
import functools

import jax
import jax.numpy as jnp
from jax import lax
from jax.experimental import pallas as pl
from jax.experimental.pallas import tpu as pltpu
from jax.sharding import PartitionSpec as P

STEPS = 8
TIME_STEP = 0.1
GRAVITY = 1.0
ROTATION = 0.2

HALF = 0.5 * TIME_STEP
SCALES = (HALF * HALF * GRAVITY, HALF, HALF)
REST = HALF * HALF * GRAVITY
TURN = TIME_STEP * ROTATION

ROWS = 128
COLS = 1024
TILES = COLS // 128
STRIP = 9
STRIPS = 16
PITCH = 9
RIM = 3
FRONT = 16
SPAN = 128 + 2 * FRONT
WORDS = SPAN * PITCH
VMEM = pltpu.VMEM


def meet(places):
    barrier = pltpu.get_barrier_semaphore()
    for where in places:
        pl.semaphore_signal(barrier, inc=1, device_id=where, device_id_type=pl.DeviceIdType.MESH)
    return barrier


def remote(k, src, dst, where, send, recv):
    return pltpu.make_async_remote_copy(
        src_ref=src, dst_ref=dst, send_sem=send.at[k], recv_sem=recv.at[k],
        device_id=where, device_id_type=pl.DeviceIdType.MESH)


def around(axis, count):
    me = lax.axis_index(axis)
    return lax.rem(me + count - 1, count), lax.rem(me + 1, count)


def rows_kernel(rows_n, x, north, south, top, bottom, send, recv):
    up, down = around("row", rows_n)
    barrier = meet([{"row": up}, {"row": down}])
    for f in range(3):
        top[f, 0:64] = x[f, 0:64]
        bottom[f, 0:64] = x[f, 8 * ROWS - 64:8 * ROWS]
        top[f, 64:72] = x[f, pl.ds(64, TILES, stride=8), :]
        bottom[f, 64:72] = x[f, pl.ds(8 * ROWS - 128 + 7, TILES, stride=8), :]
        top[f, 72:80] = jnp.zeros((8, 128), jnp.float32)
        bottom[f, 72:80] = jnp.zeros((8, 128), jnp.float32)
    pl.semaphore_wait(barrier, 2)
    copies = [remote(0, top, south, {"row": up}, send, recv), remote(1, bottom, north, {"row": down}, send, recv)]
    for copy in copies:
        copy.start()
    for copy in copies:
        copy.wait()


def swap_rows(x, rows_n):
    f32 = jnp.float32
    inside = pl.BlockSpec(memory_space=pltpu.VMEM)
    return pl.pallas_call(
        functools.partial(rows_kernel, rows_n),
        out_shape=(jax.ShapeDtypeStruct((3, 80, 128), f32), jax.ShapeDtypeStruct((3, 80, 128), f32)),
        in_specs=[inside],
        out_specs=(inside,) * 2,
        scratch_shapes=[
            VMEM((3, 80, 128), f32),
            VMEM((3, 80, 128), f32),
            pltpu.SemaphoreType.DMA((2,)),
            pltpu.SemaphoreType.DMA((2,)),
        ],
        compiler_params=pltpu.CompilerParams(collective_id=0, has_side_effects=True, vmem_limit_bytes=4 * 1024 * 1024),
    )(x)


def cut_of(q, r):
    if 0 <= r < STRIP:
        return 0, pl.ds((q + FRONT) * PITCH + r, 8, stride=PITCH)
    return 1, pl.ds((q + FRONT) * RIM + (r > 0), 8, stride=RIM)


def take(ref, q, r):
    which, cut = cut_of(q, r)
    return ref[which][cut, :]


def put(ref, q, r, value):
    which, cut = cut_of(q, r)
    ref[which][cut, :] = value


def slopes(state, q0, act):
    e_ref, u_ref, v_ref = state

    def load(r):
        e, u, v = take(e_ref, q0, r), take(u_ref, q0, r), take(v_ref, q0, r)
        return e, u, v, (e + REST) * u

    below, here = load(-1), load(0)
    for r in range(STRIP):
        above = load(r + 1)
        e, u, v, _ = here
        de, du, dv, dw = (a - b for a, b in zip(above, below))
        east, west = ((take(e_ref, q, r), take(v_ref, q, r)) for q in (q0 + 1, q0 - 1))
        ye, yv = east[0] - west[0], east[1] - west[1]
        yu = take(u_ref, q0 + 1, r) - take(u_ref, q0 - 1, r)
        ge = dw + ((east[0] + REST) * east[1] - (west[0] + REST) * west[1])
        gu = (u * du + v * (yu - TURN)) + de
        gv = (u * (dv + TURN) + v * yv) + ye
        act(r, (e, u, v), (ge, gu, gv))
        below, here = here, above


def edges(refs, q0):
    rows = [(ref, pltpu.roll(take(ref, q0, STRIP - 1), TILES, 1), pltpu.roll(take(ref, q0, 0), 128 - TILES, 1)) for ref in refs]

    def store():
        for ref, low, high in rows:
            put(ref, q0, -1, low)
            put(ref, q0, STRIP, high)

    return store


def sweep(first, blocks, work, late, unroll, opening=None):
    trips, rest = divmod(blocks, unroll)

    def trip(start, count, before, opening=None):
        stores = opening() if opening else [late(start + 8 * (k - before)) for k in range(before)]
        for k in range(count):
            work(start + 8 * k)
        for store in stores:
            store()

    trip(first, unroll, 0, opening)

    def step(i, carry):
        trip(first + 8 * unroll * i, unroll, unroll)
        return carry

    lax.fori_loop(1, trips, step, 0)
    last = first + 8 * unroll * trips
    if rest:
        trip(last, rest, unroll)
        left = [last + 8 * k for k in range(rest)]
    else:
        left = [last + 8 * (k - unroll) for k in range(unroll)]

    return lambda: [late(q) for q in left]


def run(level, a_state, b_state, c_state, d_states, out_state, origin, width, early=None):
    nothing = lambda q: lambda: None

    def keep(refs, q, r, values):
        for ref, value in zip(refs, values):
            put(ref, q, r, value)

    def blocks(reach):
        return origin - reach, (width + 2 * reach + 7) // 8

    def predict(now, then, m, with_c):
        def work(q0):
            def act(r, own, change):
                keep(then, q0, r, tuple(p - g for p, g in zip(own, change)))
                if with_c and m == 0:
                    keep(d_states[1], q0, r, tuple(p - 0.5 * g for p, g in zip(own, change)))
                elif with_c:
                    keep(c_state, q0, r, tuple(take(ref, q0, r) - 0.5 * g for ref, g in zip(d_states[m % 2], change)))

            slopes(now, q0, act)

        def late(q0):
            return edges(c_state + then if with_c and m else then, q0)

        end = m == STEPS - 1 and not with_c
        return sweep(*blocks(STEPS - m), work, nothing if end else late, 2)

    def correct(m, opening):
        def work(q0):
            def act(r, own, change):
                keep(d_states[(m + 1) % 2], q0, r, tuple(take(ref, q0, r) - g for ref, g in zip(d_states[m % 2], change)))

            slopes(c_state, q0, act)

        sweep(*blocks(STEPS - 1 - m), work, nothing, 2, opening)

    def last():
        def work(q0):
            def act(r, own, change):
                keep(out_state, q0, r, tuple(take(ref, q0, r) - 0.5 * g for ref, g in zip(d_states[0], change)))

            slopes(a_state, q0, act)

        sweep(*blocks(0), work, nothing, 2)

    def steps(with_c):
        for m in range(STEPS):
            if early is not None:
                early(with_c, m)
            now, then = (a_state, b_state) if m % 2 == 0 else (b_state, a_state)
            if m == STEPS - 1 and not with_c:
                then = out_state
            rest = predict(now, then, m, with_c)
            far = width > 64
            if not (far and with_c and m):
                for store in rest():
                    store()
            if with_c and m:
                correct(m, rest if far else None)
        if with_c:
            last()
        if early is not None:
            early(with_c, STEPS)

    @pl.when(level == 0)
    def _():
        steps(False)

    @pl.when(level == 1)
    def _():
        steps(True)


def split_state(state):
    fields, rims = list(state[:15]), list(state[15:])
    pairs = list(zip(fields[:9], rims))
    single = [(one,) for one in fields[9:]]
    return tuple(pairs[:3]), tuple(pairs[3:6]), tuple(pairs[6:9]), (tuple(single[:3]), tuple(single[3:6]))


def state_scratch(span):
    f32 = jnp.float32
    return [VMEM((span * PITCH, 128), f32) for _ in range(15)] + [VMEM((span * RIM, 128), f32) for _ in range(9)]


SEND_AHEAD = ((STEPS, 5, 5, 0), (7, 3, 3, 0))


def own_tile(x, north, south, f, c, t):
    if t == -2:
        return north[f, 57 + c:65 + c]
    if t == -1:
        return north[f, 8 * c:8 * c + 8]
    if t == ROWS // 8:
        return south[f, 8 * c:8 * c + 8]
    if t == ROWS // 8 + 1:
        return south[f, 64 + c:72 + c]
    return x[f, 64 * t + 8 * c:64 * t + 8 * c + 8]


def main_kernel(cols_n, x, north, south, sides, oe, ou, ov, side_out, send, recv, *state):
    level = lax.axis_index("level")
    west, east = around("col", cols_n)
    ids = [{"col": west}, {"col": east}]
    barrier = meet(ids)
    group = lax.rem(lax.axis_index("col"), len(SEND_AHEAD[0]))

    lane = lax.broadcasted_iota(jnp.int32, (8, 128), 1)
    view = x.reshape(3, ROWS // 8, 8 * TILES, 128)
    for k, (c, lane0) in enumerate(((0, 0), (TILES - 1, 112))):
        for f in range(3):
            whole = jnp.transpose(view[f, :, 8 * c:8 * c + 8, :].reshape(ROWS, 128))
            side_out[k, 9 * f:9 * f + 9] = whole[119:128] if k else whole[0:9]
        for j, t in enumerate((-2, -1, 16, 17)):
            out = own_tile(x, north, south, 0, c, t)
            if lane0:
                out = pltpu.roll(out, 128 - lane0, 1)
            for f in (1, 2):
                piece = pltpu.roll(own_tile(x, north, south, f, c, t), (128 - lane0 + 16 * f) % 128, 1)
                out = jnp.where(lane < 16 * f, out, piece)
            side_out[k, 32 + 8 * j:40 + 8 * j] = out
    copies = [remote(k, side_out.at[k], sides.at[k], ids[k], send, recv) for k in range(2)]

    def early(with_c, m):
        turns = SEND_AHEAD[int(with_c)]
        for k, turn in enumerate(turns):
            if turn == m:
                @pl.when(group == k)
                def _():
                    pl.semaphore_wait(barrier, 2)
                    for copy in copies:
                        copy.start()

    a_state, b_state, c_state, d_states = split_state(state)

    def tile_row(f, i):
        if i == -9:
            return north[f, 64:72]
        if i == ROWS + 8:
            return south[f, 64:72]
        if i < 0:
            return north[f, pl.ds(i + 8, TILES, stride=8), :]
        if i >= ROWS:
            return south[f, pl.ds(i - ROWS, TILES, stride=8), :]
        return x[f, pl.ds((i // 8) * 64 + i % 8, TILES, stride=8), :]

    for f, ref in enumerate(a_state):
        for r in range(-1, STRIP + 1):
            here = jnp.concatenate([tile_row(f, s * STRIP + r - 8) for s in range(STRIPS)], axis=0)
            here = jnp.transpose(here) * SCALES[f]
            for k in range(16):
                put(ref, 8 * k, r, here[8 * k:8 * k + 8])
            for q in (-16, -8, 128, 136):
                k = q % 128
                put(ref, q, r, pltpu.roll(here[k:k + 8], 1 if q < 0 else 127, 1))

    run(level, a_state, b_state, c_state, d_states, ((oe,), (ou,), (ov,)), 0, 128, early)
    for copy in copies:
        copy.wait()


def main(x, north, south, cols_n):
    f32 = jnp.float32
    inside = pl.BlockSpec(memory_space=pltpu.VMEM)
    return pl.pallas_call(
        functools.partial(main_kernel, cols_n),
        out_shape=(jax.ShapeDtypeStruct((2, 64, 128), f32),) + (jax.ShapeDtypeStruct((WORDS, 128), f32),) * 3,
        in_specs=[inside] * 3,
        out_specs=(inside,) * 4,
        scratch_shapes=[
            VMEM((2, 64, 128), f32),
            pltpu.SemaphoreType.DMA((2,)),
            pltpu.SemaphoreType.DMA((2,)),
        ] + state_scratch(SPAN),
        compiler_params=pltpu.CompilerParams(collective_id=1, has_side_effects=True, vmem_limit_bytes=32 * 1024 * 1024),
    )(x, north, south)


BAND = 9
BAND_SPAN = 64


def band_kernel(x, north, south, sides, oe, ou, ov, out, turned, beside, band, final, out_sems, be, bu, bv, *state):
    level = lax.axis_index("level")
    a_state, b_state, c_state, d_states = split_state(state)
    lane16 = lax.broadcasted_iota(jnp.int32, (16, 128), 1)
    lane8 = lax.broadcasted_iota(jnp.int32, (8, 128), 1)

    for f in range(3):
        turned[f, 0:9] = sides[0, 9 * f:9 * f + 9]
        turned[f, 119:128] = sides[1, 9 * f:9 * f + 9]
        beside[f, 16:144] = jnp.transpose(turned[f])
        for k, place in ((32, 0), (48, 144)):
            west, east = pltpu.roll(sides[1, k:k + 16], 112 - 16 * f, 1), sides[0, k:k + 16]
            if f:
                east = pltpu.roll(east, 128 - 16 * f, 1)
            beside[f, place:place + 16] = jnp.where(lane16 < 64, east, west)

    for f in range(3):
        for t in range(-2, 18):
            row = 8 * (t + 2)
            outer = beside[f, row:row + 8]
            low = pltpu.roll(jnp.where(lane8 >= 64, outer, own_tile(x, north, south, f, 0, t)), 9, 1)
            high = pltpu.roll(jnp.where(lane8 < 64, outer, own_tile(x, north, south, f, TILES - 1, t)), 82, 1)
            band[f, row:row + 8] = jnp.where(lane8 < 64, low, high)

    strip_of = lane8 % TILES
    for f, ref in enumerate(a_state):
        blocks = []
        for start in (-1, 7):
            block = [band[f, pl.ds(16 + STRIP * s - 8 + start, 8), :] for s in range(STRIPS)]
            blocks.append(jnp.transpose(jnp.concatenate(block, axis=0)) * SCALES[f])
        for r in range(-1, STRIP + 1):
            far, at = blocks[(r + 1) // 8], (r + 1) % 8
            for k in range(4):
                low, high = far[8 * k:8 * k + 8], far[64 + 8 * k:72 + 8 * k]
                if at:
                    low = pltpu.roll(low, 128 - at, 1)
                if at != TILES - 1:
                    high = pltpu.roll(high, TILES - 1 - at, 1)
                put(ref, 8 * k, r, jnp.where(strip_of == TILES - 1, high, low))

    b_out = ((be,), (bu,), (bv,))
    run(level, a_state, b_state, c_state, d_states, b_out, BAND, BAND)

    word_of = lax.broadcasted_iota(jnp.int32, (8, 128), 0)
    first, end = strip_of == 0, strip_of == TILES - 1
    done = []
    for f, (ref, fix) in enumerate(zip((oe, ou, ov), b_out)):
        for r in range(STRIP):
            block = [take((ref,), 8 * k, r) for k in range(16)]
            block[0] = jnp.where(first, take(fix, 9, r), block[0])
            block[1] = jnp.where(first & (word_of == 0), take(fix, 17, r), block[1])
            block[14] = jnp.where(end & (word_of == 7), take(fix, 2, r), block[14])
            block[15] = jnp.where(end, take(fix, 10, r), block[15])
            block = jnp.transpose(jnp.concatenate(block, axis=0)) * (1.0 / SCALES[f])
            for s in range(STRIPS):
                i = s * STRIP + r - 8
                if 0 <= i < ROWS:
                    final[f, pl.ds((i // 8) * 64 + i % 8, TILES, stride=8), :] = block[8 * s:8 * s + 8]
        done.append(pltpu.make_async_copy(final.at[f], out.at[0, f], out_sems.at[f]))
        done[-1].start()
    for copy in done:
        copy.wait()


def bands(x, *rest):
    f32 = jnp.float32
    inside = pl.BlockSpec(memory_space=pltpu.VMEM)
    return pl.pallas_call(
        band_kernel,
        out_shape=jax.ShapeDtypeStruct((1, 3, ROWS * TILES, 128), f32),
        in_specs=[inside] * 7,
        out_specs=pl.BlockSpec(memory_space=pltpu.HBM),
        scratch_shapes=[
            VMEM((3, 128, 128), f32),
            VMEM((3, 160, 128), f32),
            VMEM((3, 160, 128), f32),
            VMEM((3, ROWS * TILES, 128), f32),
            pltpu.SemaphoreType.DMA((3,)),
        ] + [VMEM((BAND_SPAN * PITCH, 128), f32) for _ in range(3)] + state_scratch(BAND_SPAN),
        compiler_params=pltpu.CompilerParams(vmem_limit_bytes=16 * 1024 * 1024),
    )(x, *rest)


def solution(mesh):
    rows_n, cols_n = mesh.shape["row"], mesh.shape["col"]

    def body(x):
        words = x.reshape(3, ROWS // 8, 8, TILES, 128).transpose(0, 1, 3, 2, 4).reshape(3, ROWS * TILES, 128)
        north, south = swap_rows(words, rows_n)
        done = bands(words, north, south, *main(words, north, south, cols_n))
        return done.reshape(1, 3, ROWS // 8, TILES, 8, 128).transpose(0, 1, 2, 4, 3, 5).reshape(1, 3, ROWS, COLS)

    return jax.shard_map(
        body,
        mesh=mesh,
        in_specs=(P(None, "row", "col"),),
        out_specs=P("level", None, "row", "col"),
        check_vma=False,
    )
```
